32 devices in a mesh: grp: 4 (over x, core), dev: 8 (over z, y).
Axes of the slice: x: 2, y: 2, z: 4, core: 2. Of those that a mesh axis runs over, the one named last changes fastest.
Arguments:
- layer_input: bfloat16 [65536, 1024], P(('grp', 'dev')), may hold values from -6 to 6
- hidden_pre: bfloat16 [65536, 1024], P(('grp', 'dev')), may hold values from -6 to 6
- out_grad: bfloat16 [65536, 512], P(('grp', 'dev')), may hold values from -6 to 6
- second_weight: bfloat16 [1024, 512], replicated, may hold values from -0.25 to 0.25
- row_grads: bfloat16 [16384, 128], P(('grp', 'dev')), may hold values from -6 to 6
- row_ids: int32 [16384], P(('grp', 'dev')), may hold values from 0 to 2047
- block_counts: int32 [256], P(('grp', 'dev')), may hold values from 1 to 64, as said below
- emb_table: float32 [16384, 128], P('dev'), may hold values from -4 to 4
- adagrad_state: float32 [16384, 128], P('dev'), may hold values from 0.01 to 1
Outputs:
- grad_first: float32 [1024, 1024], P(('grp', 'dev'))
- grad_second: float32 [1024, 512], P(('grp', 'dev'))
- new_table: float32 [16384, 128], P('dev')
- new_state: float32 [16384, 128], P('dev')
The draws below stay inside these ranges and needn't reach their ends.
Inputs may be any that keep to these rules, and one draw needn't show every extreme that they name: `block_counts`: the used slots of a block are its first ones. In every draw some owner receives full blocks of 64 used slots from every device. `row_ids`: only used slots are read.
All inputs are finite; a program needn't handle non-finite values.
Results may differ from the reference program's by a relative error of at most 0.0029.
Values may be sent and summed in bfloat16 or wider, within the bound.
A program may use at most 128 MiB of HBM per device.

```python
import math
import jax
import jax.numpy as jnp
import numpy as np
from jax import lax

IN = 1024
HID = 1024
OUT = 512
E = 128
TROWS_DEV = 2048
CAP = 64
OWNERS = 8
TOKENS = 65536
BLOCKS = 256
SLOTS = 16384
TABLE_ROWS = 16384


def draw_block_counts(key, part):
    first, second, third = jax.random.split(jax.random.fold_in(key, 11), 3)
    base = jax.random.randint(first, (BLOCKS,), 1, CAP + 1)
    heated = jax.random.randint(second, (OWNERS,), 0, 4) == 0
    forced = jax.random.randint(third, (), 0, OWNERS)
    heated = heated | (jnp.arange(OWNERS) == forced)
    owner = jnp.arange(BLOCKS) % OWNERS
    return jnp.where(heated[owner], CAP, base).astype(jnp.int32)


def place_ends(result, stream_key, least, high):
    place = [jax.random.randint(jax.random.fold_in(stream_key, axis), (), 0, length) for axis, length in enumerate(result.shape)]
    main_axis = result.shape.index(max(result.shape))
    next_to = place[:main_axis] + [(place[main_axis] + 1) % result.shape[main_axis]] + place[main_axis + 1:]
    return result.at[tuple(place)].set(least).at[tuple(next_to)].set(high)


def strengthened(array, own_key, source, target, shards_of, factor):
    def block_of(axis_at):
        return (jnp.arange(array.shape[axis_at]) // (array.shape[axis_at] // shards_of)).reshape((-1,) + (1,) * (array.ndim - 1 - axis_at))

    one_side = jax.random.permutation(own_key, shards_of)[block_of(target)]
    other_side = (block_of(target) + shards_of // 2) % shards_of
    return jnp.where((block_of(source) == one_side) | (block_of(source) == other_side), factor * array, array)


def block_levels(own_key, extent, cuts, least, high):
    loudness, own = 1.0, jax.random.fold_in(own_key, 6)
    for position, parts in cuts:
        steps = jnp.exp(jax.random.uniform(jax.random.fold_in(own, position), (parts,), jnp.float32, least / len(cuts), high / len(cuts)))
        loudness = loudness * jnp.repeat(steps, extent[position] // parts).reshape([-1 if axis == position else 1 for axis in range(len(extent))])
    return loudness


def rank_bounds(amount, skew):
    loads = [(1 << 20) // math.isqrt(standing ** skew) + 1 for standing in range(1, amount + 1)]
    width = 1 + sum(loads) // (1 << 30)
    return np.cumsum(np.array([max(1, weight // width) for weight in loads]))


def ranked_ids(stream_key, extent, amount, skew):
    listing = rank_bounds(amount, skew)
    pick = jax.random.randint(jax.random.fold_in(stream_key, 1), extent, 0, int(listing[amount - 1]))
    rank = jnp.searchsorted(jnp.asarray(listing, jnp.int32), pick, side="right")
    return jax.random.permutation(jax.random.fold_in(stream_key, 2), amount)[rank].astype(jnp.int32)


def centred(key, shape, deviation, bound, cuts=(), held_as=jnp.bfloat16):
    gain = block_levels(key, shape, cuts, -0.22, 0.18) if cuts else 1.0
    values = jax.random.normal(key, shape, jnp.float32) * deviation * gain
    return jnp.minimum(jnp.maximum(values, -bound), bound).astype(held_as)


def noise_with(key, dims, width, reach, pieces, heavy, held_as=jnp.bfloat16):
    drawn = width * jax.random.normal(key, dims, jnp.float32)
    if pieces:
        drawn = drawn * block_levels(key, dims, pieces, -0.22, 0.18)
    return jnp.clip(strengthened(drawn, jax.random.fold_in(key, 3), *heavy), -reach, reach).astype(held_as)


def setup_inputs(seed: int = 0) -> dict:
    streams_of = jax.random.split(jax.random.key(seed), 10)
    return {
        "layer_input": noise_with(streams_of[0], (TOKENS, IN), 1.0, 6.0, ((0, 32),), (0, 1, 32, 2.75)),
        "hidden_pre": noise_with(streams_of[1], (TOKENS, HID), 1.0, 6.0, ((0, 32),), (0, 1, 32, 2.75)),
        "out_grad": centred(streams_of[2], (TOKENS, OUT), 1.0, 6.0, ((0, 32),)),
        "second_weight": centred(streams_of[3], (HID, OUT), OUT ** -0.5, 0.25),
        "row_grads": centred(streams_of[4], (SLOTS, E), 1.0, 6.0, ((0, 32),)),
        "row_ids": place_ends(ranked_ids(streams_of[5], (SLOTS,), TROWS_DEV, 2), jax.random.fold_in(streams_of[5], 3), 0, TROWS_DEV - 1).astype(jnp.int32),
        "block_counts": draw_block_counts(jax.random.fold_in(streams_of[9], 71), 0),
        "emb_table": centred(streams_of[7], (TABLE_ROWS, E), 0.5, 4.0, ((0, 8),), jnp.float32),
        "adagrad_state": jnp.clip(jnp.exp(math.log(1.0) - 4.6051702 * jax.random.uniform(streams_of[8], (TABLE_ROWS, E), jnp.float32) ** block_levels(streams_of[8], (TABLE_ROWS, E), ((0, 8),), -0.2, 0.2)), 0.01, 1.0),
    }


learn_rate = 0.5
epsilon = 1e-08

def reference(layer_input, hidden_pre, out_grad, second_weight, row_grads, row_ids, block_counts, emb_table, adagrad_state):
    active = jnp.maximum(hidden_pre, jnp.zeros_like(hidden_pre))
    back = jnp.dot(out_grad, second_weight.T, preferred_element_type=jnp.float32)
    d_hidden = (back * (hidden_pre > 0).astype(jnp.float32)).astype(jnp.bfloat16)
    contract = (((0,), (0,)), ((), ()))
    grad_first = lax.dot_general(layer_input, d_hidden, contract, preferred_element_type=jnp.float32)
    grad_second = lax.dot_general(active, out_grad, contract, preferred_element_type=jnp.float32)
    slot_index = jnp.arange(row_grads.shape[0], dtype=jnp.int32)
    block_index = slot_index // CAP
    owner = block_index % OWNERS
    usable = slot_index % CAP < block_counts[block_index]
    target = owner * TROWS_DEV + row_ids
    values = row_grads.astype(jnp.float32) * usable.astype(jnp.float32)[:, None]
    table_grad = jax.ops.segment_sum(values, target, num_segments=TABLE_ROWS)
    new_state = adagrad_state + table_grad * table_grad
    new_table = emb_table - learn_rate * table_grad / (jnp.sqrt(new_state) + epsilon)
    return (grad_first, grad_second, new_table, new_state)
```

```python
import functools

import jax
import jax.numpy as jnp
from jax import lax
from jax.experimental import pallas as pl
from jax.experimental.pallas import tpu as pltpu
from jax.sharding import PartitionSpec as P

learn_rate = 0.5
epsilon = 1e-08
MESH = pl.DeviceIdType.MESH
LANES = 128
f32, bf16 = jnp.float32, jnp.bfloat16


def kernel(
    G, D, PW,
    x_hbm, h_hbm, og_hbm, w2_hbm, rg_hbm, ids_hbm, cnt_hbm, tab_hbm, st_hbm,
    g1_ref, g2_ref, tab_ref, st_ref,
    x_v, h_v, og_v, w2_v, dh_v, tab_v, st_v, ids_v, cnt_s,
    hv, cs, cr, xs, xr, ys, yr, fv, zs, zr,
    sb, eb, eo, ij, ir, ib, iz, io,
    lsem, cs_s, cr_s, xs_s, xr_s, ys_s, yr_s, zs_s, zr_s,
    es_s, er_s, ez_s, ez_r,
):
    GX, DH = G // 2, D // 2
    assert GX == 2
    g, d = lax.axis_index("grp"), lax.axis_index("dev")
    gx, c = g // 2, g % 2
    dh, dl = d // 2, d % 2
    tokens = x_v.shape[0]
    n1, n2 = dh_v.shape[1], og_v.shape[1]
    R = g1_ref.shape[0]
    DR = D * R
    first_core = c == 0

    def pick(a, b):
        return jnp.where(first_core, a, b)

    def local(src, dst, i):
        return pltpu.make_async_copy(src, dst, lsem.at[i])

    half = tokens // 2
    other_c = (c + 1) % 2

    def group_cols(gxx, cc):
        return pl.ds(pl.multiple_of((gxx * 2 + cc) * DR, DR), DR)

    loads = {}

    def load(name, src, dst):
        copy = local(src, dst, len(loads))
        loads[name] = copy
        copy.start()

    load("ids", ids_hbm, ids_v)
    load("cnt", cnt_hbm, cnt_s)
    load("og", og_hbm, og_v)
    for k in range(GX):
        load(("h", "a", k), h_hbm.at[:, group_cols(k, other_c)], h_v.at[:, group_cols(k, other_c)])
    for k in range(GX):
        load(("h", "h", k), h_hbm.at[:, group_cols(k, c)], h_v.at[:, group_cols(k, c)])
    load("w2", w2_hbm, w2_v)
    load("x", x_hbm, x_v)
    load("own", rg_hbm.at[:, dl], sb.at[:, 0, dl])
    load("tab", tab_hbm, tab_v)
    load("st", st_hbm, st_v)

    odl = (dl + 1) % 2
    core_peer = (gx * 2 + other_c, d)
    x_peer = (((gx + 1) % GX) * 2 + c, d)
    y_peer = (g, dh * 2 + odl)
    line = [(k, ((dh + k) % DH) * 2 + dl) for k in range(1, DH)]
    first_peer = (pick(x_peer[0], y_peer[0]), pick(x_peer[1], y_peer[1]))
    second_peer = (pick(y_peer[0], x_peer[0]), pick(y_peer[1], x_peer[1]))
    peers = [core_peer, x_peer, y_peer] + [(g, pd) for k, pd in line]
    barrier = pltpu.get_barrier_semaphore()
    for peer in peers:
        pl.semaphore_signal(barrier, inc=1, device_id=peer, device_id_type=MESH)

    loads["ids"].wait()
    loads["cnt"].wait()
    lane = lax.broadcasted_iota(jnp.int32, (1, LANES), 1)
    side = lane // (LANES // 2)
    for z in range(DH):
        count = jnp.where(side == 0, cnt_s[2 * z], cnt_s[2 * z + 1])
        row = jnp.where(lane % (LANES // 2) < count, ids_v[z : z + 1, :], -1)
        ib[z, 0] = jnp.where(side == dl, row, -1)
        ij[z] = pltpu.roll(jnp.where(side == odl, row, -1), LANES // 2, 1)

    pl.semaphore_wait(barrier, len(peers))

    def remote(src, dst, ss, rs, to):
        return pltpu.make_async_remote_copy(
            src_ref=src, dst_ref=dst, send_sem=ss, recv_sem=rs, device_id=to, device_id_type=MESH
        )

    pending = []

    def send(*args):
        copy = remote(*args)
        copy.start()
        pending.append(copy)

    def landed(dst, ss, rs):
        remote(dst, dst, ss, rs, core_peer).wait_recv()

    send(rg_hbm.at[:, odl], sb.at[:, 0, dl], es_s.at[0], er_s.at[0], y_peer)
    send(ij, ir, es_s.at[1], er_s.at[1], y_peer)
    send(rg_hbm.at[:, dl], sb.at[:, 1, dl], es_s.at[2], er_s.at[2], x_peer)

    def slots_x():
        landed(sb.at[:, 0, odl], es_s.at[0], er_s.at[0])
        landed(ir, es_s.at[1], er_s.at[1])
        for z in range(DH):
            ib[z, 0] = jnp.maximum(ib[z, 0], ir[z])
        send(ib.at[:, 0], ib.at[:, 1], es_s.at[3], er_s.at[3], x_peer)
        send(sb.at[:, 0, odl], sb.at[:, 1, odl], es_s.at[4], er_s.at[4], x_peer)

    def slots_z():
        loads["own"].wait()
        landed(ib.at[:, 1], es_s.at[3], er_s.at[3])
        landed(sb.at[:, 1, dl], es_s.at[2], er_s.at[2])
        landed(sb.at[:, 1, odl], es_s.at[4], er_s.at[4])
        for k, pd in line[::-1]:
            t = (dh + k) % DH
            send(ib.at[t], iz.at[k], ez_s.at[0, k], ez_r.at[0, k], (g, pd))
            send(sb.at[t], eb.at[k], ez_s.at[1, k], ez_r.at[1, k], (g, pd))
        send(ib.at[dh], io.at[0], es_s.at[5], er_s.at[5], core_peer)
        send(sb.at[dh], eo.at[0], es_s.at[6], er_s.at[6], core_peer)

    def slots_core():
        for k, pd in line:
            landed(iz.at[k], ez_s.at[0, k], ez_r.at[0, k])
            landed(eb.at[k], ez_s.at[1, k], ez_r.at[1, k])
        rest = pl.ds(1, DH - 1)
        send(iz.at[rest], io.at[rest], es_s.at[7], er_s.at[7], core_peer)
        send(eb.at[rest], eo.at[rest], es_s.at[8], er_s.at[8], core_peer)

    def slots_all():
        landed(io.at[0], es_s.at[5], er_s.at[5])
        landed(eo.at[0], es_s.at[6], er_s.at[6])
        rest = pl.ds(1, DH - 1)
        landed(io.at[rest], es_s.at[7], er_s.at[7])
        landed(eo.at[rest], es_s.at[8], er_s.at[8])

    contract = (((0,), (0,)), ((), ()))

    def left(src, cc, relu):
        block = jnp.concatenate([src[:, group_cols(k, cc)] for k in range(GX)], axis=1)
        if relu:
            block = jnp.maximum(block, jnp.zeros_like(block))
        return block

    def away(n, width, src, relu, rhs, at):
        value = lax.dot_general(
            left(src, other_c, relu), rhs[:, at : at + width], contract, preferred_element_type=f32
        )
        for s in range(width // PW):
            for k in range(GX):
                cs[n + s, k] = value[k * DR : (k + 1) * DR, s * PW : (s + 1) * PW]
            send(cs.at[n + s], cr.at[n + s], cs_s.at[n + s], cr_s.at[n + s], core_peer)

    def home(n, width, src, relu, rhs, at):
        value = lax.dot_general(
            left(src, c, relu), rhs[:, at : at + width], contract, preferred_element_type=f32
        )
        for s in range(width // PW):
            for k in range(GX):
                hv[n + s, k] = value[k * DR : (k + 1) * DR, s * PW : (s + 1) * PW]

    p_me, q_me = pick(gx, dl), pick(dl, gx)
    p_no, q_no = 1 - p_me, 1 - q_me

    def chip_sum(n, p, q, b):
        k = pick(p, q)
        rows = pl.ds(pl.multiple_of((b * 2 + pick(q, p)) * R, R), R)
        return hv[n, k, rows, :] + cr[n, k, rows, :]

    def step_chip(n):
        landed(cr.at[n], cs_s.at[n], cr_s.at[n])
        for q in range(2):
            for b in range(DH):
                xs[n, q, b] = chip_sum(n, p_no, q, b).astype(bf16)
        send(xs.at[n], xr.at[n], xs_s.at[n], xr_s.at[n], first_peer)

    def step_first(n):
        landed(xr.at[n], xs_s.at[n], xr_s.at[n])
        for b in range(DH):
            ys[n, b] = (chip_sum(n, p_me, q_no, b) + xr[n, q_no, b].astype(f32)).astype(bf16)
        send(ys.at[n], yr.at[n], ys_s.at[n], yr_s.at[n], second_peer)
        for b in range(DH):
            fv[n, b] = chip_sum(n, p_me, q_me, b) + xr[n, q_me, b].astype(f32)

    def step_second(n):
        landed(yr.at[n], ys_s.at[n], yr_s.at[n])
        for b in range(DH):
            value = fv[n, b] + yr[n, b].astype(f32)
            zs[n, b] = value.astype(bf16)
            fv[n, b] = value
        for k, pd in line[::-1]:
            send(zs.at[n, (dh + k) % DH], zr.at[n, k], zs_s.at[n, k], zr_s.at[n, k], (g, pd))

    def step_line(n, out, at):
        value = fv[n, dh]
        for k, pd in line:
            landed(zr.at[n, k], zs_s.at[n, k], zr_s.at[n, k])
            value = value + zr[n, k].astype(f32)
        out[:, at : at + PW] = value

    def back(rows, cols):
        value = lax.dot_general(
            og_v[rows, :], w2_v[cols, :], (((1,), (1,)), ((), ())), preferred_element_type=f32
        )
        keep = h_v[rows, cols].astype(f32) > 0
        dh_v[rows, cols] = jnp.where(keep, value, jnp.zeros_like(value)).astype(bf16)

    owned = tab_v.shape[0]
    tile = 256

    def table_tiles(first, last):
        def body(t, _):
            start = pl.multiple_of(t * tile, tile)
            rows = pl.ds(start, tile)
            wanted = start + lax.broadcasted_iota(jnp.int32, (tile, LANES), 0)
            total = jnp.zeros((tile, tab_v.shape[1]), f32)
            for k in range(DH):
                parts = []
                blocks = []
                for who in range(2):
                    for a in range(GX):
                        if who:
                            ids, block = io[k, a], eo[k, a]
                        elif k:
                            ids, block = iz[k, a], eb[k, a]
                        else:
                            ids, block = ib[dh, a], sb[dh, a]
                        hit = wanted == ids
                        parts.append(jnp.where(hit, 1.0, 0.0).astype(bf16))
                        blocks.append(block.reshape(LANES, tab_v.shape[1]))
                total = total + jnp.dot(
                    jnp.concatenate(parts, axis=1),
                    jnp.concatenate(blocks, axis=0),
                    preferred_element_type=f32,
                )
            state = st_v[rows, :] + total * total
            st_ref[rows, :] = state
            tab_ref[rows, :] = tab_v[rows, :] - learn_rate * total / (jnp.sqrt(state) + epsilon)
            return 0

        lax.fori_loop(first, last, body, 0)

    W = 2 * PW
    loads["og"].wait()
    for k in range(GX):
        loads[("h", "a", k)].wait()
    away(0, W, h_v, True, og_v, 0)
    for k in range(GX):
        loads[("h", "h", k)].wait()
    home(0, W, h_v, True, og_v, 0)
    loads["w2"].wait()
    back(pl.ds(0, half), pl.ds(0, W))
    slots_x()
    step_chip(0)
    step_chip(1)
    back(pl.ds(half, half), pl.ds(0, W))
    loads["x"].wait()
    away(2, W, x_v, False, dh_v, 0)
    home(2, W, x_v, False, dh_v, 0)
    slots_z()
    back(pl.ds(0, half), pl.ds(W, W))
    step_chip(2)
    step_chip(3)
    step_first(0)
    back(pl.ds(half, half), pl.ds(W, W))
    step_first(1)
    away(4, W, x_v, False, dh_v, W)
    home(4, W, x_v, False, dh_v, W)
    step_chip(4)
    step_chip(5)
    step_second(0)
    step_first(2)
    slots_core()
    step_second(1)
    step_first(3)
    step_second(2)
    loads["tab"].wait()
    loads["st"].wait()
    slots_all()
    tiles = owned // tile
    table_tiles(0, tiles // 2)
    step_first(4)
    step_second(3)
    table_tiles(tiles // 2, tiles)
    step_first(5)
    step_second(4)
    step_line(0, g2_ref, 0)
    step_line(1, g2_ref, PW)
    step_second(5)
    step_line(2, g1_ref, 0)
    step_line(3, g1_ref, PW)
    step_line(4, g1_ref, W)
    step_line(5, g1_ref, W + PW)
    for copy in pending:
        copy.wait_send()


def solution(mesh):
    G, D = mesh.shape["grp"], mesh.shape["dev"]

    def on_device(
        layer_input, hidden_pre, out_grad, second_weight,
        row_grads, row_ids, block_counts, emb_table, adagrad_state,
    ):
        T, IN = layer_input.shape
        HID, OUT = second_weight.shape
        E = row_grads.shape[1]
        cap = row_grads.shape[0] // D
        assert LANES // cap == 2
        GX, DH = G // 2, D // 2
        R1, R2 = IN // (G * D), HID // (G * D)
        PW = OUT // 2
        N = (OUT + HID) // PW
        hbm = pl.BlockSpec(memory_space=pltpu.HBM)
        vmem = pl.BlockSpec(memory_space=pltpu.VMEM)
        dma = pltpu.SemaphoreType.DMA
        return pl.pallas_call(
            functools.partial(kernel, G, D, PW),
            out_shape=[
                jax.ShapeDtypeStruct((R1, HID), f32),
                jax.ShapeDtypeStruct((R2, OUT), f32),
                jax.ShapeDtypeStruct(emb_table.shape, f32),
                jax.ShapeDtypeStruct(adagrad_state.shape, f32),
            ],
            in_specs=[hbm] * 9,
            out_specs=[vmem] * 4,
            scratch_shapes=[
                pltpu.VMEM((T, IN), bf16),
                pltpu.VMEM((T, HID), bf16),
                pltpu.VMEM((T, OUT), bf16),
                pltpu.VMEM((HID, OUT), bf16),
                pltpu.VMEM((T, HID), bf16),
                pltpu.VMEM(emb_table.shape, f32),
                pltpu.VMEM(adagrad_state.shape, f32),
                pltpu.VMEM((DH, LANES), jnp.int32),
                pltpu.SMEM((D,), jnp.int32),
                pltpu.VMEM((N, GX, D * R1, PW), f32),
                pltpu.VMEM((N, GX, D * R1, PW), f32),
                pltpu.VMEM((N, GX, D * R1, PW), f32),
                pltpu.VMEM((N, 2, DH, R1, PW), bf16),
                pltpu.VMEM((N, 2, DH, R1, PW), bf16),
                pltpu.VMEM((N, DH, R1, PW), bf16),
                pltpu.VMEM((N, DH, R1, PW), bf16),
                pltpu.VMEM((N, DH, R1, PW), f32),
                pltpu.VMEM((N, DH, R1, PW), bf16),
                pltpu.VMEM((N, DH, R1, PW), bf16),
                pltpu.VMEM((DH, GX, 2, cap, E), bf16),
                pltpu.VMEM((DH, GX, 2, cap, E), bf16),
                pltpu.VMEM((DH, GX, 2, cap, E), bf16),
                pltpu.VMEM((DH, 1, LANES), jnp.int32),
                pltpu.VMEM((DH, 1, LANES), jnp.int32),
                pltpu.VMEM((DH, GX, 1, LANES), jnp.int32),
                pltpu.VMEM((DH, GX, 1, LANES), jnp.int32),
                pltpu.VMEM((DH, GX, 1, LANES), jnp.int32),
                dma((16,)),
                dma((N,)), dma((N,)),
                dma((N,)), dma((N,)),
                dma((N,)), dma((N,)),
                dma((N, DH)), dma((N, DH)),
                dma((9,)), dma((9,)),
                dma((2, DH)), dma((2, DH)),
            ],
            compiler_params=pltpu.CompilerParams(
                collective_id=0, has_side_effects=True, vmem_limit_bytes=52 * 1024 * 1024
            ),
        )(
            layer_input, hidden_pre, out_grad, second_weight,
            row_grads.reshape(DH, 2, cap, E), row_ids.reshape(DH, LANES), block_counts,
            emb_table, adagrad_state,
        )

    return jax.shard_map(
        on_device,
        mesh=mesh,
        in_specs=(
            P(("grp", "dev"), None),
            P(("grp", "dev"), None),
            P(("grp", "dev"), None),
            P(),
            P(("grp", "dev"), None),
            P(("grp", "dev")),
            P(("grp", "dev")),
            P("dev", None),
            P("dev", None),
        ),
        out_specs=(P(("grp", "dev"), None), P(("grp", "dev"), None), P("dev", None), P("dev", None)),
        check_vma=False,
    )
```

```python
import functools

import jax
import jax.numpy as jnp
from jax import lax
from jax.experimental import pallas as pl
from jax.experimental.pallas import tpu as pltpu
from jax.sharding import PartitionSpec as P

learn_rate = 0.5
epsilon = 1e-08
MESH = pl.DeviceIdType.MESH
LANES = 128
f32, bf16 = jnp.float32, jnp.bfloat16


def kernel(
    G, D,
    x_hbm, h_hbm, og_hbm, w2_hbm, rg_hbm, ids_hbm, cnt_hbm, tab_hbm, st_hbm,
    g1_ref, g2_ref, tab_ref, st_ref,
    x_v, h_v, og_v, w2_v, dh_v, ids_v, cnt_s,
    hv, cs, cr, xs, xr, ys, yr, fv, zs, zr,
    sb, eb, eo, ij, iw, iz, io,
    sums, lsem, s_sem, c_sem, x_sem, y_sem, z_sem, e_sem,
):
    GX, DH = G // 2, D // 2
    assert GX == 2
    g, d = lax.axis_index("grp"), lax.axis_index("dev")
    gx, c = g // 2, g % 2
    dh, dl = d // 2, d % 2
    tokens = x_v.shape[0]
    half = tokens // 2
    R = g1_ref.shape[0]
    DR = D * R
    U = LANES
    first_core = c == 0

    def pick(a, b):
        return jnp.where(first_core, a, b)

    other_c = (c + 1) % 2

    def group_cols(k, cc):
        return pl.ds(pl.multiple_of((k * 2 + cc) * DR, DR), DR)

    loads = {}

    def load(name, src, dst):
        copy = pltpu.make_async_copy(src, dst, lsem.at[len(loads)])
        loads[name] = copy
        copy.start()

    load("ids", ids_hbm, ids_v)
    load("cnt", cnt_hbm, cnt_s)
    for t in range(2):
        rows = pl.ds(t * half, half)
        load(("og", t), og_hbm.at[rows], og_v.at[rows])
        for k in range(GX):
            cols = group_cols(k, other_c)
            load(("h", "away", t, k), h_hbm.at[rows, cols], h_v.at[rows, cols])
    for k in range(GX):
        cols = group_cols(k, c)
        load(("h", "home", k), h_hbm.at[:, cols], h_v.at[:, cols])
    load("w2", w2_hbm, w2_v)
    load("x", x_hbm, x_v)
    load("own", rg_hbm.at[:, dl], sb.at[:, gx, dl])
    load("tab", tab_hbm, tab_ref)
    load("st", st_hbm, st_ref)

    odl = (dl + 1) % 2
    core_peer = (gx * 2 + other_c, d)
    x_peer = (((gx + 1) % GX) * 2 + c, d)
    y_peer = (g, dh * 2 + odl)
    diagonal = (x_peer[0], y_peer[1])
    line = [(k, ((dh + k) % DH) * 2 + dl) for k in range(1, DH)]
    first_peer = (pick(x_peer[0], y_peer[0]), pick(x_peer[1], y_peer[1]))
    second_peer = (pick(y_peer[0], x_peer[0]), pick(y_peer[1], x_peer[1]))
    peers = [core_peer, x_peer, y_peer, diagonal] + [(g, pd) for k, pd in line]
    barrier = pltpu.get_barrier_semaphore()
    for peer in peers:
        pl.semaphore_signal(barrier, inc=1, device_id=peer, device_id_type=MESH)

    loads["ids"].wait()
    loads["cnt"].wait()
    lane = lax.broadcasted_iota(jnp.int32, (1, LANES), 1)
    side = lane // (LANES // 2)
    for z in range(DH):
        count = jnp.where(side == 0, cnt_s[2 * z], cnt_s[2 * z + 1])
        row = jnp.where(lane % (LANES // 2) < count, ids_v[z : z + 1, :], -1)
        ij[0, z] = jnp.where(side == dl, row, -1)
        ij[1, z] = pltpu.roll(jnp.where(side == odl, row, -1), LANES // 2, 1)
        iw[z, gx, dl] = ij[0, z]

    pl.semaphore_wait(barrier, len(peers))

    def remote(src, dst, ss, rs, to):
        return pltpu.make_async_remote_copy(
            src_ref=src, dst_ref=dst, send_sem=ss, recv_sem=rs, device_id=to, device_id_type=MESH
        )

    def send(src, dst, i, rs, to):
        remote(src, dst, s_sem.at[i], rs, to).start()

    def landed(dst, rs):
        remote(dst, dst, s_sem.at[8], rs, core_peer).wait_recv()

    def left_here(src, i):
        remote(src, src, s_sem.at[i], c_sem.at[0], core_peer).wait_send()

    ox = (gx + 1) % GX
    plane = [(y_peer, odl, gx, odl, 1), (x_peer, dl, ox, dl, 0), (diagonal, odl, ox, odl, 1)]
    for i, (to, y, _, _, moved) in enumerate(plane):
        send(ij.at[moved], iw.at[:, gx, dl], 2 * i, e_sem.at[2 * i], to)
        send(rg_hbm.at[:, y], sb.at[:, gx, dl], 2 * i + 1, e_sem.at[2 * i + 1], to)

    def slots_line():
        loads["own"].wait()
        for i, (_, _, a, b, _) in enumerate(plane):
            landed(iw.at[:, a, b], e_sem.at[2 * i])
            landed(sb.at[:, a, b], e_sem.at[2 * i + 1])
        for k, pd in line[::-1]:
            t = (dh + k) % DH
            send(iw.at[t], iz.at[k], 12, e_sem.at[6], (g, pd))
            send(sb.at[t], eb.at[k], 13, e_sem.at[7], (g, pd))
        send(iw.at[dh], io.at[0], 14, e_sem.at[8], core_peer)
        send(sb.at[dh], eo.at[0], 15, e_sem.at[9], core_peer)

    rest = pl.ds(1, DH - 1)

    def slots_core():
        landed(iz.at[rest], e_sem.at[6])
        landed(eb.at[rest], e_sem.at[7])
        send(iz.at[rest], io.at[rest], 16, e_sem.at[10], core_peer)
        send(eb.at[rest], eo.at[rest], 17, e_sem.at[11], core_peer)

    def slots_here(a):
        landed(io.at[rest if a else 0], e_sem.at[8 + 2 * a])
        landed(eo.at[rest if a else 0], e_sem.at[9 + 2 * a])

    contract = (((0,), (0,)), ((), ()))

    def left(src, cc, relu, rows):
        block = jnp.concatenate([src[rows, group_cols(k, cc)] for k in range(GX)], axis=1)
        if relu:
            block = jnp.maximum(block, jnp.zeros_like(block))
        return block

    def product(dst, cc, n, units, src, relu, rhs, at, rows=pl.ds(0, tokens), add=False):
        cols = pl.ds(at * U if isinstance(at, int) else pl.multiple_of(at * U, U), units * U)
        value = lax.dot_general(
            left(src, cc, relu, rows), rhs[rows, cols], contract, preferred_element_type=f32
        )
        for s in range(units):
            for k in range(GX):
                part = value[k * DR : (k + 1) * DR, s * U : (s + 1) * U]
                dst[n + s, k] = dst[n + s, k] + part if add else part

    def send_core(j, n, w):
        p = pl.ds(n, w)
        send(cs.at[p], cr.at[p], 8, c_sem.at[j], core_peer)

    def away_two(j, n, src, rhs, at):
        def body(i, _):
            product(cs, other_c, n + 2 * i, 2, src, False, rhs, at + 2 * i)
            send_core(j + i, n + 2 * i, 2)
            return 0

        lax.fori_loop(0, 2, body, 0)

    p_me, q_me = pick(gx, dl), pick(dl, gx)
    p_no, q_no = 1 - p_me, 1 - q_me

    def chip_sum(n, p, q, b):
        k = pick(p, q)
        rows = pl.ds(pl.multiple_of((b * 2 + pick(q, p)) * R, R), R)
        return hv[n, k, rows, :] + cr[n, k, rows, :]

    pieces = [(0, 2), (2, 2), (4, 2), (6, 2), (8, 2), (10, 1), (11, 1)]

    def chip_landed(j, n, w):
        landed(cr.at[pl.ds(n, w)], c_sem.at[j])

    def step_chip(j):
        n, w = pieces[j]
        at = pl.ds(n, w)
        for u in range(n, n + w):
            for q in range(2):
                for b in range(DH):
                    xs[u, q, b] = chip_sum(u, p_no, q, b).astype(bf16)
        send(xs.at[at], xr.at[at], 9, x_sem.at[j], first_peer)

    def step_first(j):
        n, w = pieces[j]
        at = pl.ds(n, w)
        landed(xr.at[at], x_sem.at[j])
        for u in range(n, n + w):
            for b in range(DH):
                ys[u, b] = (chip_sum(u, p_me, q_no, b) + xr[u, q_no, b].astype(f32)).astype(bf16)
        send(ys.at[at], yr.at[at], 10, y_sem.at[j], second_peer)
        for u in range(n, n + w):
            for b in range(DH):
                fv[u, b] = chip_sum(u, p_me, q_me, b) + xr[u, q_me, b].astype(f32)

    def step_second(j):
        n, w = pieces[j]
        at = pl.ds(n, w)
        landed(yr.at[at], y_sem.at[j])
        for b in range(DH):
            for u in range(n, n + w):
                value = fv[u, b] + yr[u, b].astype(f32)
                zs[b, u] = value.astype(bf16)
                fv[u, b] = value
        for k, pd in line[::-1]:
            send(zs.at[(dh + k) % DH, at], zr.at[k, at], 11, z_sem.at[j], (g, pd))

    def step_line(j):
        n, w = pieces[j]
        landed(zr.at[pl.ds(1, DH - 1), pl.ds(n, w)], z_sem.at[j])
        for u in range(n, n + w):
            value = fv[u, dh]
            for k, pd in line:
                value = value + zr[k, u].astype(f32)
            if u < n2:
                g2_ref[:, u * U : (u + 1) * U] = value
            else:
                g1_ref[:, (u - n2) * U : (u - n2 + 1) * U] = value

    def back(rows, at, units):
        cols = pl.ds(at * U, units * U)
        value = lax.dot_general(
            og_v[rows, :], w2_v[cols, :], (((1,), (1,)), ((), ())), preferred_element_type=f32
        )
        keep = h_v[rows, cols].astype(f32) > 0
        dh_v[rows, cols] = jnp.where(keep, value, jnp.zeros_like(value)).astype(bf16)

    E = tab_ref.shape[1]
    tile = 256
    every = pl.ds(0, tokens)

    def table_tiles(a, first, last):
        def body(t, _):
            start = pl.multiple_of(t * tile, tile)
            rows = pl.ds(start, tile)
            wanted = start + lax.broadcasted_iota(jnp.int32, (tile, LANES), 0)
            total = sums[rows, :] if a else jnp.zeros((tile, E), f32)
            for k in range(1, DH) if a else range(1):
                parts, blocks = [], []
                for ids, block in ((iz[k], eb[k]) if k else (iw[dh], sb[dh]), (io[k], eo[k])):
                    for e in range(GX):
                        hit = wanted == jnp.maximum(ids[e, 0], ids[e, 1])
                        parts.append(jnp.where(hit, 1.0, 0.0).astype(bf16))
                    blocks.append(block.reshape(GX * LANES, E))
                total = total + jnp.dot(
                    jnp.concatenate(parts, axis=1),
                    jnp.concatenate(blocks, axis=0),
                    preferred_element_type=f32,
                )
            if not a:
                sums[rows, :] = total
            else:
                state = st_ref[rows, :] + total * total
                st_ref[rows, :] = state
                tab_ref[rows, :] = tab_ref[rows, :] - learn_rate * total / (jnp.sqrt(state) + epsilon)
            return 0

        lax.fori_loop(first, last, body, 0)

    tiles = tab_ref.shape[0] // tile
    some = tiles // 4
    n2 = og_v.shape[1] // U
    n1 = dh_v.shape[1] // U
    assert n2 == 4 and n1 == 8
    loads[("og", 0)].wait()
    for k in range(GX):
        loads[("h", "away", 0, k)].wait()
    product(cs, other_c, 0, 4, h_v, True, og_v, 0, pl.ds(0, half))
    loads[("og", 1)].wait()
    for k in range(GX):
        loads[("h", "away", 1, k)].wait()
    product(cs, other_c, 0, 4, h_v, True, og_v, 0, pl.ds(half, half), True)
    send_core(0, 0, 2)
    send_core(1, 2, 2)
    for k in range(GX):
        loads[("h", "home", k)].wait()
    product(hv, c, 0, 4, h_v, True, og_v, 0)
    chip_landed(0, 0, 2)
    step_chip(0)
    loads["w2"].wait()
    back(every, 0, 4)
    chip_landed(1, 2, 2)
    step_chip(1)
    loads["x"].wait()
    away_two(2, 4, x_v, dh_v, 0)
    slots_line()
    product(hv, c, 4, 4, x_v, False, dh_v, 0)
    chip_landed(2, 4, 2)
    step_chip(2)
    step_first(0)
    back(every, 4, 4)
    chip_landed(3, 6, 2)
    step_chip(3)
    step_first(1)
    away_two(4, 8, x_v, dh_v, 4)
    product(hv, c, 8, 4, x_v, False, dh_v, 4)
    chip_landed(4, 8, 2)
    step_chip(4)
    step_second(0)
    step_first(2)
    chip_landed(5, 10, 2)
    step_chip(5)
    step_chip(6)
    step_second(1)
    slots_here(0)
    table_tiles(0, 0, 4 * some)
    step_first(3)
    step_second(2)
    slots_core()
    loads["tab"].wait()
    loads["st"].wait()
    step_first(4)
    slots_here(1)
    table_tiles(1, 0, some)
    step_first(5)
    step_second(3)
    table_tiles(1, some, 2 * some)
    step_first(6)
    step_second(4)
    table_tiles(1, 2 * some, 3 * some)
    step_second(5)
    table_tiles(1, 3 * some, tiles)
    step_second(6)
    for j in range(7):
        step_line(j)
    for i in range(3):
        left_here(ij.at[0], 2 * i)
        left_here(sb.at[:, 0, 0], 2 * i + 1)
    left_here(iz.at[rest], 12)
    left_here(eb.at[rest], 13)
    left_here(iz.at[0], 14)
    left_here(eb.at[0], 15)
    left_here(iz.at[rest], 16)
    left_here(eb.at[rest], 17)
    left_here(cs, 8)
    left_here(xs, 9)
    left_here(ys, 10)
    left_here(zs.at[pl.ds(1, DH - 1)], 11)


def store(*refs):
    ins, outs, sems = refs[:4], refs[4:8], refs[8]
    copies = [pltpu.make_async_copy(a, b, sems.at[i]) for i, (a, b) in enumerate(zip(ins, outs))]
    for copy in copies:
        copy.start()
    for copy in copies:
        copy.wait()


def solution(mesh):
    G, D = mesh.shape["grp"], mesh.shape["dev"]

    def on_device(
        layer_input, hidden_pre, out_grad, second_weight,
        row_grads, row_ids, block_counts, emb_table, adagrad_state,
    ):
        T, IN = layer_input.shape
        HID, OUT = second_weight.shape
        E = row_grads.shape[1]
        cap = row_grads.shape[0] // D
        assert LANES // cap == 2
        GX, DH = G // 2, D // 2
        R1, R2 = IN // (G * D), HID // (G * D)
        assert R1 == R2
        U = LANES
        N = (OUT + HID) // U
        hbm = pl.BlockSpec(memory_space=pltpu.HBM)
        vmem = pl.BlockSpec(memory_space=pltpu.VMEM)
        dma = pltpu.SemaphoreType.DMA
        operands = (
            layer_input, hidden_pre, out_grad, second_weight,
            row_grads.reshape(DH, 2, cap, E), row_ids.reshape(DH, LANES), block_counts,
            emb_table, adagrad_state,
        )
        grads = pl.pallas_call(
            functools.partial(kernel, G, D),
            out_shape=[
                jax.ShapeDtypeStruct((R1, HID), f32),
                jax.ShapeDtypeStruct((R2, OUT), f32),
                jax.ShapeDtypeStruct(emb_table.shape, f32),
                jax.ShapeDtypeStruct(adagrad_state.shape, f32),
            ],
            in_specs=[hbm] * 9,
            out_specs=[vmem] * 4,
            scratch_shapes=[
                pltpu.VMEM((T, IN), bf16),
                pltpu.VMEM((T, HID), bf16),
                pltpu.VMEM((T, OUT), bf16),
                pltpu.VMEM((HID, OUT), bf16),
                pltpu.VMEM((T, HID), bf16),
                pltpu.VMEM((DH, LANES), jnp.int32),
                pltpu.SMEM((D,), jnp.int32),
                pltpu.VMEM((N, GX, D * R1, U), f32),
                pltpu.VMEM((N, GX, D * R1, U), f32),
                pltpu.VMEM((N, GX, D * R1, U), f32),
                pltpu.VMEM((N, 2, DH, R1, U), bf16),
                pltpu.VMEM((N, 2, DH, R1, U), bf16),
                pltpu.VMEM((N, DH, R1, U), bf16),
                pltpu.VMEM((N, DH, R1, U), bf16),
                pltpu.VMEM((N, DH, R1, U), f32),
                pltpu.VMEM((DH, N, R1, U), bf16),
                pltpu.VMEM((DH, N, R1, U), bf16),
                pltpu.VMEM((DH, GX, 2, cap, E), bf16),
                pltpu.VMEM((DH, GX, 2, cap, E), bf16),
                pltpu.VMEM((DH, GX, 2, cap, E), bf16),
                pltpu.VMEM((2, DH, 1, LANES), jnp.int32),
                pltpu.VMEM((DH, GX, 2, 1, LANES), jnp.int32),
                pltpu.VMEM((DH, GX, 2, 1, LANES), jnp.int32),
                pltpu.VMEM((DH, GX, 2, 1, LANES), jnp.int32),
                pltpu.VMEM(emb_table.shape, f32),
                dma((15,)),
                dma((18,)),
                dma((6,)), dma((7,)), dma((7,)), dma((7,)),
                dma((12,)),
            ],
            compiler_params=pltpu.CompilerParams(
                collective_id=0, has_side_effects=True, vmem_limit_bytes=48 * 1024 * 1024
            ),
        )(*[pltpu.with_memory_space_constraint(a, pltpu.HBM) for a in operands])
        return pl.pallas_call(
            store,
            out_shape=[jax.ShapeDtypeStruct(a.shape, a.dtype) for a in grads],
            in_specs=[vmem] * 4,
            out_specs=[hbm] * 4,
            scratch_shapes=[dma((4,))],
            compiler_params=pltpu.CompilerParams(vmem_limit_bytes=8 * 1024 * 1024),
        )(*grads)

    return jax.shard_map(
        on_device,
        mesh=mesh,
        in_specs=(
            P(("grp", "dev"), None),
            P(("grp", "dev"), None),
            P(("grp", "dev"), None),
            P(),
            P(("grp", "dev"), None),
            P(("grp", "dev")),
            P(("grp", "dev")),
            P("dev", None),
            P("dev", None),
        ),
        out_specs=(P(("grp", "dev"), None), P(("grp", "dev"), None), P("dev", None), P("dev", None)),
        check_vma=False,
    )
```

```python
import functools

import jax
import jax.numpy as jnp
from jax import lax
from jax.experimental import pallas as pl
from jax.experimental.pallas import tpu as pltpu
from jax.sharding import PartitionSpec as P

learn_rate = 0.5
epsilon = 1e-08
MESH = pl.DeviceIdType.MESH
LANES = 128
f32, bf16 = jnp.float32, jnp.bfloat16


def kernel(
    G, D,
    x_hbm, h_hbm, og_hbm, w2_hbm, rg_hbm, ids_hbm, cnt_hbm, tab_hbm, st_hbm,
    g1_ref, g2_ref, tab_ref, st_ref,
    x_v, h_v, og_v, w2_v, dh_v, ids_v, cnt_s,
    hv, cs, cr, xs, xr, ys, yr, fv, zs, zr, ds, dr, zx, zy, fz, px, py,
    sb, eb, eo, ij, iw, iz, io,
    sums, lsem, s_sem, c_sem, x_sem, y_sem, z_sem, e_sem, d_sem,
):
    GX, DH = G // 2, D // 2
    assert GX == 2
    g, d = lax.axis_index("grp"), lax.axis_index("dev")
    gx, c = g // 2, g % 2
    dh, dl = d // 2, d % 2
    tokens = x_v.shape[0]
    half = tokens // 2
    R = g1_ref.shape[0]
    DR = D * R
    U = LANES
    first_core = c == 0

    def pick(a, b):
        return jnp.where(first_core, a, b)

    other_c = (c + 1) % 2

    def group_cols(k, cc):
        return pl.ds(pl.multiple_of((k * 2 + cc) * DR, DR), DR)

    loads = {}

    def load(name, src, dst):
        copy = pltpu.make_async_copy(src, dst, lsem.at[len(loads)])
        loads[name] = copy
        copy.start()

    load("ids", ids_hbm, ids_v)
    load("cnt", cnt_hbm, cnt_s)
    for t in range(2):
        rows = pl.ds(t * half, half)
        load(("og", t), og_hbm.at[rows], og_v.at[rows])
        for k in range(GX):
            cols = group_cols(k, other_c)
            load(("h", "away", t, k), h_hbm.at[rows, cols], h_v.at[rows, cols])
    for k in range(GX):
        cols = group_cols(k, c)
        load(("h", "home", k), h_hbm.at[:, cols], h_v.at[:, cols])
    load("w2", w2_hbm, w2_v)
    load("x", x_hbm, x_v)
    load("own", rg_hbm.at[:, dl], sb.at[:, gx, dl])
    load("tab", tab_hbm, tab_ref)
    load("st", st_hbm, st_ref)

    odl = (dl + 1) % 2
    core_peer = (gx * 2 + other_c, d)
    x_peer = (((gx + 1) % GX) * 2 + c, d)
    y_peer = (g, dh * 2 + odl)
    diagonal = (x_peer[0], y_peer[1])
    line = [(k, ((dh + k) % DH) * 2 + dl) for k in range(1, DH)]
    first_peer = (pick(x_peer[0], y_peer[0]), pick(x_peer[1], y_peer[1]))
    second_peer = (pick(y_peer[0], x_peer[0]), pick(y_peer[1], x_peer[1]))
    peers = [core_peer, x_peer, y_peer, diagonal] + [(g, pd) for k, pd in line]
    barrier = pltpu.get_barrier_semaphore()
    for peer in peers:
        pl.semaphore_signal(barrier, inc=1, device_id=peer, device_id_type=MESH)

    loads["ids"].wait()
    loads["cnt"].wait()
    lane = lax.broadcasted_iota(jnp.int32, (1, LANES), 1)
    side = lane // (LANES // 2)
    for z in range(DH):
        count = jnp.where(side == 0, cnt_s[2 * z], cnt_s[2 * z + 1])
        row = jnp.where(lane % (LANES // 2) < count, ids_v[z : z + 1, :], -1)
        ij[0, z] = jnp.where(side == dl, row, -1)
        ij[1, z] = pltpu.roll(jnp.where(side == odl, row, -1), LANES // 2, 1)
        iw[z, gx, dl] = ij[0, z]

    pl.semaphore_wait(barrier, len(peers))

    def remote(src, dst, ss, rs, to):
        return pltpu.make_async_remote_copy(
            src_ref=src, dst_ref=dst, send_sem=ss, recv_sem=rs, device_id=to, device_id_type=MESH
        )

    def send(src, dst, i, rs, to):
        remote(src, dst, s_sem.at[i], rs, to).start()

    def landed(dst, rs):
        remote(dst, dst, s_sem.at[8], rs, core_peer).wait_recv()

    def left_here(src, i):
        remote(src, src, s_sem.at[i], c_sem.at[0], core_peer).wait_send()

    ox = (gx + 1) % GX
    plane = [(y_peer, odl, gx, odl, 1), (x_peer, dl, ox, dl, 0), (diagonal, odl, ox, odl, 1)]
    for i, (to, y, _, _, moved) in enumerate(plane):
        send(ij.at[moved], iw.at[:, gx, dl], 2 * i, e_sem.at[2 * i], to)
        send(rg_hbm.at[:, y], sb.at[:, gx, dl], 2 * i + 1, e_sem.at[2 * i + 1], to)

    def slots_line():
        loads["own"].wait()
        for i, (_, _, a, b, _) in enumerate(plane):
            landed(iw.at[:, a, b], e_sem.at[2 * i])
            landed(sb.at[:, a, b], e_sem.at[2 * i + 1])
        for k, pd in line[::-1]:
            t = (dh + k) % DH
            send(iw.at[t], iz.at[k], 12, e_sem.at[6], (g, pd))
            send(sb.at[t], eb.at[k], 13, e_sem.at[7], (g, pd))
        send(iw.at[dh], io.at[0], 14, e_sem.at[8], core_peer)
        send(sb.at[dh], eo.at[0], 15, e_sem.at[9], core_peer)

    rest = pl.ds(1, DH - 1)

    def slots_core():
        landed(iz.at[rest], e_sem.at[6])
        landed(eb.at[rest], e_sem.at[7])
        send(iz.at[rest], io.at[rest], 16, e_sem.at[10], core_peer)
        send(eb.at[rest], eo.at[rest], 17, e_sem.at[11], core_peer)

    def slots_here(a):
        landed(io.at[rest if a else 0], e_sem.at[8 + 2 * a])
        landed(eo.at[rest if a else 0], e_sem.at[9 + 2 * a])

    contract = (((0,), (0,)), ((), ()))

    def left(src, cc, relu, rows):
        block = jnp.concatenate([src[rows, group_cols(k, cc)] for k in range(GX)], axis=1)
        if relu:
            block = jnp.maximum(block, jnp.zeros_like(block))
        return block

    def product(dst, cc, n, units, src, relu, rhs, at, rows=pl.ds(0, tokens), add=False):
        cols = pl.ds(at * U if isinstance(at, int) else pl.multiple_of(at * U, U), units * U)
        value = lax.dot_general(
            left(src, cc, relu, rows), rhs[rows, cols], contract, preferred_element_type=f32
        )
        for s in range(units):
            for k in range(GX):
                part = value[k * DR : (k + 1) * DR, s * U : (s + 1) * U]
                dst[n + s, k] = dst[n + s, k] + part if add else part

    def send_core(j, n, w):
        p = pl.ds(n, w)
        send(cs.at[p], cr.at[p], 8, c_sem.at[j], core_peer)

    def away_two(j, n, src, rhs, at):
        def body(i, _):
            product(cs, other_c, n + 2 * i, 2, src, False, rhs, at + 2 * i)
            send_core(j + i, n + 2 * i, 2)
            return 0

        lax.fori_loop(0, 2, body, 0)

    p_me, q_me = pick(gx, dl), pick(dl, gx)
    p_no, q_no = 1 - p_me, 1 - q_me

    def chip_sum(n, p, q, b):
        k = pick(p, q)
        rows = pl.ds(pl.multiple_of((b * 2 + pick(q, p)) * R, R), R)
        return hv[n, k, rows, :] + cr[n, k, rows, :]

    pieces = [(0, 2), (2, 2), (4, 2), (6, 2), (8, 1), (9, 1), (10, 1), (11, 1)]
    late, over_z = 6, [7]
    units = [sum(w for j, (_, w) in enumerate(pieces) if j not in skip) for skip in (over_z + [late], over_z)]

    def chip_landed(j, n, w):
        landed(cr.at[pl.ds(n, w)], c_sem.at[j])

    def step_chip(j):
        n, w = pieces[j]
        at = pl.ds(n, w)
        for u in range(n, n + w):
            for q in range(2):
                for b in range(DH):
                    xs[u, q, b] = chip_sum(u, p_no, q, b).astype(bf16)
        send(xs.at[at], xr.at[at], 9, x_sem.at[j], first_peer)

    def step_first(j):
        n, w = pieces[j]
        at = pl.ds(n, w)
        landed(xr.at[at], x_sem.at[j])
        for u in range(n, n + w):
            for b in range(DH):
                ys[u, b] = (chip_sum(u, p_me, q_no, b) + xr[u, q_no, b].astype(f32)).astype(bf16)
        send(ys.at[at], yr.at[at], 10, y_sem.at[j], second_peer)
        for u in range(n, n + w):
            for b in range(DH):
                fv[u, b] = chip_sum(u, p_me, q_me, b) + xr[u, q_me, b].astype(f32)

    def step_plane(j):
        n, w = pieces[j]
        for i, (p, q, to) in enumerate(
            ((p_no, q_no, diagonal), (p_no, q_me, first_peer), (p_me, q_no, second_peer))
        ):
            for u in range(w):
                for b in range(DH):
                    ds[i, j - late, u, b] = chip_sum(n + u, p, q, b).astype(bf16)
            send(ds.at[i, j - late], dr.at[i, j - late], 18, d_sem.at[i, j - late], to)

    def plane_landed(j):
        n, w = pieces[j]
        for i in range(1, 4):
            landed(dr.at[i % 3, j - late], d_sem.at[i % 3, j - late])
        for b in range(DH):
            for u in range(w):
                value = chip_sum(n + u, p_me, q_me, b)
                for i in range(3):
                    value = value + dr[i, j - late, u, b].astype(f32)
                zs[b, n + u] = value.astype(bf16)
                fv[n + u, b] = value
        for k, pd in line[::-1]:
            at = pl.ds(n, w)
            send(zs.at[(dh + k) % DH, at], zr.at[k, at], 11, z_sem.at[j], (g, pd))

    def line_first(j):
        n, _ = pieces[j]
        o = over_z.index(j)
        for b in range(DH):
            for p in range(2):
                for q in range(2):
                    zx[o, b, p, q] = chip_sum(n, p, q, b).astype(bf16)
        for k, pd in line[::-1]:
            send(zx.at[o, (dh + k) % DH], zy.at[o, k], 19, z_sem.at[j], (g, pd))

    def line_plane(j):
        n, _ = pieces[j]
        o = over_z.index(j)
        landed(zy.at[o, pl.ds(1, DH - 1)], z_sem.at[j])

        def line_sum(p, q):
            value = chip_sum(n, p, q, dh)
            for k, pd in line:
                value = value + zy[o, k, p, q].astype(f32)
            return value

        for i, (p, q, to) in enumerate(
            ((p_no, q_no, diagonal), (p_no, q_me, first_peer), (p_me, q_no, second_peer))
        ):
            px[o, i] = line_sum(p, q).astype(bf16)
            send(px.at[o, i], py.at[o, i], 20, d_sem.at[i, 1 + o], to)
        fz[o] = line_sum(p_me, q_me)

    def line_end(j):
        n, _ = pieces[j]
        o = over_z.index(j)
        value = fz[o]
        for i in range(3):
            landed(py.at[o, i], d_sem.at[i, 1 + o])
            value = value + py[o, i].astype(f32)
        g1_ref[:, (n - n2) * U : (n - n2 + 1) * U] = value

    def step_second(j):
        n, w = pieces[j]
        at = pl.ds(n, w)
        landed(yr.at[at], y_sem.at[j])
        for b in range(DH):
            for u in range(n, n + w):
                value = fv[u, b] + yr[u, b].astype(f32)
                zs[b, u] = value.astype(bf16)
                fv[u, b] = value
        for k, pd in line[::-1]:
            send(zs.at[(dh + k) % DH, at], zr.at[k, at], 11, z_sem.at[j], (g, pd))

    def step_line(j):
        n, w = pieces[j]
        landed(zr.at[pl.ds(1, DH - 1), pl.ds(n, w)], z_sem.at[j])
        for u in range(n, n + w):
            value = fv[u, dh]
            for k, pd in line:
                value = value + zr[k, u].astype(f32)
            if u < n2:
                g2_ref[:, u * U : (u + 1) * U] = value
            else:
                g1_ref[:, (u - n2) * U : (u - n2 + 1) * U] = value

    def back(rows, at, units):
        cols = pl.ds(at * U, units * U)
        value = lax.dot_general(
            og_v[rows, :], w2_v[cols, :], (((1,), (1,)), ((), ())), preferred_element_type=f32
        )
        keep = h_v[rows, cols].astype(f32) > 0
        dh_v[rows, cols] = jnp.where(keep, value, jnp.zeros_like(value)).astype(bf16)

    E = tab_ref.shape[1]
    tile = 256
    every = pl.ds(0, tokens)

    def table_tiles(a, first, last):
        def body(t, _):
            start = pl.multiple_of(t * tile, tile)
            rows = pl.ds(start, tile)
            wanted = start + lax.broadcasted_iota(jnp.int32, (tile, LANES), 0)
            total = sums[rows, :] if a else jnp.zeros((tile, E), f32)
            for k in range(1, DH) if a else range(1):
                parts, blocks = [], []
                for ids, block in ((iz[k], eb[k]) if k else (iw[dh], sb[dh]), (io[k], eo[k])):
                    for e in range(GX):
                        hit = wanted == jnp.maximum(ids[e, 0], ids[e, 1])
                        parts.append(jnp.where(hit, 1.0, 0.0).astype(bf16))
                    blocks.append(block.reshape(GX * LANES, E))
                total = total + jnp.dot(
                    jnp.concatenate(parts, axis=1),
                    jnp.concatenate(blocks, axis=0),
                    preferred_element_type=f32,
                )
            if not a:
                sums[rows, :] = total
            else:
                state = st_ref[rows, :] + total * total
                st_ref[rows, :] = state
                tab_ref[rows, :] = tab_ref[rows, :] - learn_rate * total / (jnp.sqrt(state) + epsilon)
            return 0

        lax.fori_loop(first, last, body, 0)

    tiles = tab_ref.shape[0] // tile
    some = tiles // 4
    n2 = og_v.shape[1] // U
    n1 = dh_v.shape[1] // U
    assert n2 == 4 and n1 == 8
    loads[("og", 0)].wait()
    for k in range(GX):
        loads[("h", "away", 0, k)].wait()
    product(cs, other_c, 0, 4, h_v, True, og_v, 0, pl.ds(0, half))
    loads[("og", 1)].wait()
    for k in range(GX):
        loads[("h", "away", 1, k)].wait()
    product(cs, other_c, 0, 4, h_v, True, og_v, 0, pl.ds(half, half), True)
    send_core(0, 0, 2)
    send_core(1, 2, 2)
    for k in range(GX):
        loads[("h", "home", k)].wait()
    product(hv, c, 0, 4, h_v, True, og_v, 0)
    chip_landed(0, 0, 2)
    step_chip(0)
    loads["w2"].wait()
    back(every, 0, 4)
    chip_landed(1, 2, 2)
    step_chip(1)
    loads["x"].wait()
    away_two(2, 4, x_v, dh_v, 0)
    slots_line()
    product(hv, c, 4, 4, x_v, False, dh_v, 0)
    chip_landed(2, 4, 2)
    step_chip(2)
    step_first(0)
    back(every, 4, 4)
    chip_landed(3, 6, 2)
    step_chip(3)
    step_first(1)
    away_two(4, 8, x_v, dh_v, 4)
    product(hv, c, 8, 4, x_v, False, dh_v, 4)
    chip_landed(4, 8, 2)
    step_chip(4)
    step_chip(5)
    chip_landed(5, 10, 2)
    step_plane(6)
    line_first(7)
    step_first(2)
    step_second(0)
    step_second(1)
    slots_here(0)
    table_tiles(0, 0, 2 * some)
    step_first(3)
    table_tiles(0, 2 * some, 4 * some)
    slots_core()
    step_first(4)
    step_first(5)
    step_second(2)
    loads["tab"].wait()
    loads["st"].wait()
    step_second(3)
    plane_landed(6)
    step_second(4)
    line_plane(7)
    step_second(5)
    slots_here(1)
    table_tiles(1, 0, tiles)
    for j in range(7):
        step_line(j)
    line_end(7)
    for i in range(3):
        left_here(ij.at[0], 2 * i)
        left_here(sb.at[:, 0, 0], 2 * i + 1)
    left_here(iz.at[rest], 12)
    left_here(eb.at[rest], 13)
    left_here(iz.at[0], 14)
    left_here(eb.at[0], 15)
    left_here(iz.at[rest], 16)
    left_here(eb.at[rest], 17)
    left_here(cs, 8)
    left_here(xs.at[pl.ds(0, units[0])], 9)
    left_here(ys.at[pl.ds(0, units[0])], 10)
    left_here(ds, 18)
    left_here(zx.at[:, pl.ds(1, DH - 1)], 19)
    left_here(px, 20)
    left_here(zs.at[pl.ds(1, DH - 1), pl.ds(0, units[1])], 11)


def store(*refs):
    ins, outs, sems = refs[:4], refs[4:8], refs[8]
    copies = [pltpu.make_async_copy(a, b, sems.at[i]) for i, (a, b) in enumerate(zip(ins, outs))]
    for copy in copies:
        copy.start()
    for copy in copies:
        copy.wait()


def solution(mesh):
    G, D = mesh.shape["grp"], mesh.shape["dev"]

    def on_device(
        layer_input, hidden_pre, out_grad, second_weight,
        row_grads, row_ids, block_counts, emb_table, adagrad_state,
    ):
        T, IN = layer_input.shape
        HID, OUT = second_weight.shape
        E = row_grads.shape[1]
        cap = row_grads.shape[0] // D
        assert LANES // cap == 2
        GX, DH = G // 2, D // 2
        R1, R2 = IN // (G * D), HID // (G * D)
        assert R1 == R2
        U = LANES
        N = (OUT + HID) // U
        hbm = pl.BlockSpec(memory_space=pltpu.HBM)
        vmem = pl.BlockSpec(memory_space=pltpu.VMEM)
        dma = pltpu.SemaphoreType.DMA
        operands = (
            layer_input, hidden_pre, out_grad, second_weight,
            row_grads.reshape(DH, 2, cap, E), row_ids.reshape(DH, LANES), block_counts,
            emb_table, adagrad_state,
        )
        grads = pl.pallas_call(
            functools.partial(kernel, G, D),
            out_shape=[
                jax.ShapeDtypeStruct((R1, HID), f32),
                jax.ShapeDtypeStruct((R2, OUT), f32),
                jax.ShapeDtypeStruct(emb_table.shape, f32),
                jax.ShapeDtypeStruct(adagrad_state.shape, f32),
            ],
            in_specs=[hbm] * 9,
            out_specs=[vmem] * 4,
            scratch_shapes=[
                pltpu.VMEM((T, IN), bf16),
                pltpu.VMEM((T, HID), bf16),
                pltpu.VMEM((T, OUT), bf16),
                pltpu.VMEM((HID, OUT), bf16),
                pltpu.VMEM((T, HID), bf16),
                pltpu.VMEM((DH, LANES), jnp.int32),
                pltpu.SMEM((D,), jnp.int32),
                pltpu.VMEM((N, GX, D * R1, U), f32),
                pltpu.VMEM((N, GX, D * R1, U), f32),
                pltpu.VMEM((N, GX, D * R1, U), f32),
                pltpu.VMEM((N, 2, DH, R1, U), bf16),
                pltpu.VMEM((N, 2, DH, R1, U), bf16),
                pltpu.VMEM((N, DH, R1, U), bf16),
                pltpu.VMEM((N, DH, R1, U), bf16),
                pltpu.VMEM((N, DH, R1, U), f32),
                pltpu.VMEM((DH, N, R1, U), bf16),
                pltpu.VMEM((DH, N, R1, U), bf16),
                pltpu.VMEM((3, 1, 1, DH, R1, U), bf16),
                pltpu.VMEM((3, 1, 1, DH, R1, U), bf16),
                pltpu.VMEM((1, DH, 2, 2, R1, U), bf16),
                pltpu.VMEM((1, DH, 2, 2, R1, U), bf16),
                pltpu.VMEM((1, R1, U), f32),
                pltpu.VMEM((1, 3, R1, U), bf16),
                pltpu.VMEM((1, 3, R1, U), bf16),
                pltpu.VMEM((DH, GX, 2, cap, E), bf16),
                pltpu.VMEM((DH, GX, 2, cap, E), bf16),
                pltpu.VMEM((DH, GX, 2, cap, E), bf16),
                pltpu.VMEM((2, DH, 1, LANES), jnp.int32),
                pltpu.VMEM((DH, GX, 2, 1, LANES), jnp.int32),
                pltpu.VMEM((DH, GX, 2, 1, LANES), jnp.int32),
                pltpu.VMEM((DH, GX, 2, 1, LANES), jnp.int32),
                pltpu.VMEM(emb_table.shape, f32),
                dma((15,)),
                dma((21,)),
                dma((6,)), dma((8,)), dma((8,)), dma((8,)),
                dma((12,)),
                dma((3, 1 + 1)),
            ],
            compiler_params=pltpu.CompilerParams(
                collective_id=0, has_side_effects=True, vmem_limit_bytes=48 * 1024 * 1024
            ),
        )(*[pltpu.with_memory_space_constraint(a, pltpu.HBM) for a in operands])
        return pl.pallas_call(
            store,
            out_shape=[jax.ShapeDtypeStruct(a.shape, a.dtype) for a in grads],
            in_specs=[vmem] * 4,
            out_specs=[hbm] * 4,
            scratch_shapes=[dma((4,))],
            compiler_params=pltpu.CompilerParams(vmem_limit_bytes=8 * 1024 * 1024),
        )(*grads)

    return jax.shard_map(
        on_device,
        mesh=mesh,
        in_specs=(
            P(("grp", "dev"), None),
            P(("grp", "dev"), None),
            P(("grp", "dev"), None),
            P(),
            P(("grp", "dev"), None),
            P(("grp", "dev")),
            P(("grp", "dev")),
            P("dev", None),
            P("dev", None),
        ),
        out_specs=(P(("grp", "dev"), None), P(("grp", "dev"), None), P("dev", None), P("dev", None)),
        check_vma=False,
    )
```

```python
import functools

import jax
import jax.numpy as jnp
from jax import lax
from jax.experimental import pallas as pl
from jax.experimental.pallas import tpu as pltpu
from jax.sharding import PartitionSpec as P

learn_rate = 0.5
epsilon = 1e-08
MESH = pl.DeviceIdType.MESH
LANES = 128
f32, bf16 = jnp.float32, jnp.bfloat16


def kernel(
    G, D,
    x_hbm, h_hbm, og_hbm, w2_hbm, rg_hbm, ids_hbm, cnt_hbm, tab_hbm, st_hbm,
    g1_ref, g2_ref, tab_ref, st_ref,
    x_v, h_v, og_v, w2_v, dh_v, ids_v, cnt_s,
    hv, cs, cr, xs, xr, ys, yr, fv, zs, zr, ds, dr, zx, zy, fz, px, py,
    sb, eb, eo, ij, iw, iz, io,
    sums, lsem, s_sem, c_sem, x_sem, y_sem, z_sem, e_sem, d_sem,
):
    GX, DH = G // 2, D // 2
    assert GX == 2
    g, d = lax.axis_index("grp"), lax.axis_index("dev")
    gx, c = g // 2, g % 2
    dh, dl = d // 2, d % 2
    tokens = x_v.shape[0]
    half = tokens // 2
    R = g1_ref.shape[0]
    DR = D * R
    U = LANES
    first_core = c == 0

    def pick(a, b):
        return jnp.where(first_core, a, b)

    other_c = (c + 1) % 2

    def group_cols(k, cc):
        return pl.ds(pl.multiple_of((k * 2 + cc) * DR, DR), DR)

    loads = {}

    def load(name, src, dst):
        copy = pltpu.make_async_copy(src, dst, lsem.at[len(loads)])
        loads[name] = copy
        copy.start()

    load("ids", ids_hbm, ids_v)
    load("cnt", cnt_hbm, cnt_s)
    for t in range(2):
        rows = pl.ds(t * half, half)
        load(("og", t), og_hbm.at[rows], og_v.at[rows])
        for k in range(GX):
            cols = group_cols(k, other_c)
            load(("h", "away", t, k), h_hbm.at[rows, cols], h_v.at[rows, cols])
    for k in range(GX):
        cols = group_cols(k, c)
        load(("h", "home", k), h_hbm.at[:, cols], h_v.at[:, cols])
    load("w2", w2_hbm, w2_v)
    load("x", x_hbm, x_v)
    load("own", rg_hbm.at[:, dl], sb.at[:, gx, dl])
    load("tab", tab_hbm, tab_ref)
    load("st", st_hbm, st_ref)

    odl = (dl + 1) % 2
    core_peer = (gx * 2 + other_c, d)
    x_peer = (((gx + 1) % GX) * 2 + c, d)
    y_peer = (g, dh * 2 + odl)
    diagonal = (x_peer[0], y_peer[1])
    line = [(k, ((dh + k) % DH) * 2 + dl) for k in range(1, DH)]
    first_peer = (pick(x_peer[0], y_peer[0]), pick(x_peer[1], y_peer[1]))
    second_peer = (pick(y_peer[0], x_peer[0]), pick(y_peer[1], x_peer[1]))
    peers = [core_peer, x_peer, y_peer, diagonal] + [(g, pd) for k, pd in line]
    barrier = pltpu.get_barrier_semaphore()
    for peer in peers:
        pl.semaphore_signal(barrier, inc=1, device_id=peer, device_id_type=MESH)

    loads["ids"].wait()
    loads["cnt"].wait()
    lane = lax.broadcasted_iota(jnp.int32, (1, LANES), 1)
    side = lane // (LANES // 2)
    for z in range(DH):
        count = jnp.where(side == 0, cnt_s[2 * z], cnt_s[2 * z + 1])
        row = jnp.where(lane % (LANES // 2) < count, ids_v[z : z + 1, :], -1)
        ij[0, z] = jnp.where(side == dl, row, -1)
        ij[1, z] = pltpu.roll(jnp.where(side == odl, row, -1), LANES // 2, 1)
        iw[z, gx, dl] = ij[0, z]

    pl.semaphore_wait(barrier, len(peers))

    def remote(src, dst, ss, rs, to):
        return pltpu.make_async_remote_copy(
            src_ref=src, dst_ref=dst, send_sem=ss, recv_sem=rs, device_id=to, device_id_type=MESH
        )

    def send(src, dst, i, rs, to):
        remote(src, dst, s_sem.at[i], rs, to).start()

    def landed(dst, rs):
        remote(dst, dst, s_sem.at[8], rs, core_peer).wait_recv()

    def left_here(src, i):
        remote(src, src, s_sem.at[i], c_sem.at[0], core_peer).wait_send()

    ox = (gx + 1) % GX
    plane = [(y_peer, odl, gx, odl, 1), (x_peer, dl, ox, dl, 0), (diagonal, odl, ox, odl, 1)]
    for i, (to, y, _, _, moved) in enumerate(plane):
        send(ij.at[moved], iw.at[:, gx, dl], 2 * i, e_sem.at[2 * i], to)
        send(rg_hbm.at[:, y], sb.at[:, gx, dl], 2 * i + 1, e_sem.at[2 * i + 1], to)
    for k, pd in line[::-1]:
        t = (dh + k) % DH
        send(ij.at[0, t], iz.at[k, gx, dl], 12, e_sem.at[6], (g, pd))
        send(rg_hbm.at[t, dl], eb.at[k, gx, dl], 13, e_sem.at[7], (g, pd))

    def slots_line():
        loads["own"].wait()
        for i, (_, _, a, b, _) in enumerate(plane):
            landed(iw.at[:, a, b], e_sem.at[2 * i])
            landed(sb.at[:, a, b], e_sem.at[2 * i + 1])
        for k, pd in line[::-1]:
            t = (dh + k) % DH
            for at in ((gx, odl), (ox,)):
                send(iw.at[(t, *at)], iz.at[(k, *at)], 12, e_sem.at[6], (g, pd))
                send(sb.at[(t, *at)], eb.at[(k, *at)], 13, e_sem.at[7], (g, pd))
        send(iw.at[dh], io.at[0], 14, e_sem.at[8], core_peer)
        send(sb.at[dh], eo.at[0], 15, e_sem.at[9], core_peer)

    rest = pl.ds(1, DH - 1)

    def slots_core():
        landed(iz.at[rest], e_sem.at[6])
        landed(eb.at[rest], e_sem.at[7])
        send(iz.at[rest], io.at[rest], 16, e_sem.at[10], core_peer)
        send(eb.at[rest], eo.at[rest], 17, e_sem.at[11], core_peer)

    def slots_here(a):
        landed(io.at[rest if a else 0], e_sem.at[8 + 2 * a])
        landed(eo.at[rest if a else 0], e_sem.at[9 + 2 * a])

    contract = (((0,), (0,)), ((), ()))

    def left(src, cc, relu, rows):
        block = jnp.concatenate([src[rows, group_cols(k, cc)] for k in range(GX)], axis=1)
        if relu:
            block = jnp.maximum(block, jnp.zeros_like(block))
        return block

    def product(dst, cc, n, units, src, relu, rhs, at, rows=pl.ds(0, tokens), add=False):
        cols = pl.ds(at * U if isinstance(at, int) else pl.multiple_of(at * U, U), units * U)
        value = lax.dot_general(
            left(src, cc, relu, rows), rhs[rows, cols], contract, preferred_element_type=f32
        )
        for s in range(units):
            for k in range(GX):
                part = value[k * DR : (k + 1) * DR, s * U : (s + 1) * U]
                dst[n + s, k] = dst[n + s, k] + part if add else part

    def send_core(j, n, w):
        p = pl.ds(n, w)
        send(cs.at[p], cr.at[p], 8, c_sem.at[j], core_peer)

    def away_two(j, n, src, rhs, at):
        def body(i, _):
            product(cs, other_c, n + 2 * i, 2, src, False, rhs, at + 2 * i)
            send_core(j + i, n + 2 * i, 2)
            return 0

        lax.fori_loop(0, 2, body, 0)

    def home_two(n, src, rhs, at, after):
        def body(i, _):
            product(hv, c, n + 2 * i, 2, src, False, rhs, at + 2 * i)
            for k in range(2):
                pl.when(i == k)(after[k])
            return 0

        lax.fori_loop(0, 2, body, 0)

    p_me, q_me = pick(gx, dl), pick(dl, gx)
    p_no, q_no = 1 - p_me, 1 - q_me

    def chip_sum(n, p, q, b):
        k = pick(p, q)
        rows = pl.ds(pl.multiple_of((b * 2 + pick(q, p)) * R, R), R)
        return hv[n, k, rows, :] + cr[n, k, rows, :]

    pieces = [(0, 2), (2, 1), (4, 2), (6, 2), (8, 1), (9, 1), (10, 1), (11, 1), (3, 1)]
    late, over_z = 6, [7, 8]
    units = [sum(w for j, (_, w) in enumerate(pieces) if j not in skip) for skip in (over_z + [late], over_z)]

    def chip_landed(j, n, w):
        landed(cr.at[pl.ds(n, w)], c_sem.at[j])

    def step_chip(j):
        n, w = pieces[j]
        at = pl.ds(n, w)
        for u in range(n, n + w):
            for q in range(2):
                for b in range(DH):
                    xs[u, q, b] = chip_sum(u, p_no, q, b).astype(bf16)
        send(xs.at[at], xr.at[at], 9, x_sem.at[j], first_peer)

    def step_first(j):
        n, w = pieces[j]
        at = pl.ds(n, w)
        landed(xr.at[at], x_sem.at[j])
        for u in range(n, n + w):
            for b in range(DH):
                ys[u, b] = (chip_sum(u, p_me, q_no, b) + xr[u, q_no, b].astype(f32)).astype(bf16)
        send(ys.at[at], yr.at[at], 10, y_sem.at[j], second_peer)
        for u in range(n, n + w):
            for b in range(DH):
                fv[u, b] = chip_sum(u, p_me, q_me, b) + xr[u, q_me, b].astype(f32)

    def step_plane(j):
        n, w = pieces[j]
        for i, (p, q, to) in enumerate(
            ((p_no, q_no, diagonal), (p_no, q_me, first_peer), (p_me, q_no, second_peer))
        ):
            for u in range(w):
                for b in range(DH):
                    ds[i, j - late, u, b] = chip_sum(n + u, p, q, b).astype(bf16)
            send(ds.at[i, j - late], dr.at[i, j - late], 18, d_sem.at[i, j - late], to)

    def plane_landed(j):
        n, w = pieces[j]
        for i in range(1, 4):
            landed(dr.at[i % 3, j - late], d_sem.at[i % 3, j - late])
        for b in range(DH):
            for u in range(w):
                value = chip_sum(n + u, p_me, q_me, b)
                for i in range(3):
                    value = value + dr[i, j - late, u, b].astype(f32)
                zs[b, n + u] = value.astype(bf16)
                fv[n + u, b] = value
        for k, pd in line[::-1]:
            at = pl.ds(n, w)
            send(zs.at[(dh + k) % DH, at], zr.at[k, at], 11, z_sem.at[j], (g, pd))

    def line_first(j):
        n, _ = pieces[j]
        o = over_z.index(j)
        for b in range(DH):
            for p in range(2):
                for q in range(2):
                    zx[o, b, p, q] = chip_sum(n, p, q, b).astype(bf16)
        for k, pd in line[::-1]:
            send(zx.at[o, (dh + k) % DH], zy.at[o, k], 19, z_sem.at[j], (g, pd))

    def line_plane(j):
        n, _ = pieces[j]
        o = over_z.index(j)
        landed(zy.at[o, pl.ds(1, DH - 1)], z_sem.at[j])

        def line_sum(p, q):
            value = chip_sum(n, p, q, dh)
            for k, pd in line:
                value = value + zy[o, k, p, q].astype(f32)
            return value

        for i, (p, q, to) in enumerate(
            ((p_no, q_no, diagonal), (p_no, q_me, first_peer), (p_me, q_no, second_peer))
        ):
            px[o, i] = line_sum(p, q).astype(bf16)
            send(px.at[o, i], py.at[o, i], 20, d_sem.at[i, 1 + o], to)
        fz[o] = line_sum(p_me, q_me)

    def line_end(j):
        n, _ = pieces[j]
        o = over_z.index(j)
        value = fz[o]
        for i in range(3):
            landed(py.at[o, i], d_sem.at[i, 1 + o])
            value = value + py[o, i].astype(f32)
        out, at = (g2_ref, n) if n < n2 else (g1_ref, n - n2)
        out[:, at * U : (at + 1) * U] = value

    def step_second(j):
        n, w = pieces[j]
        at = pl.ds(n, w)
        landed(yr.at[at], y_sem.at[j])
        for b in range(DH):
            for u in range(n, n + w):
                value = fv[u, b] + yr[u, b].astype(f32)
                zs[b, u] = value.astype(bf16)
                fv[u, b] = value
        for k, pd in line[::-1]:
            send(zs.at[(dh + k) % DH, at], zr.at[k, at], 11, z_sem.at[j], (g, pd))

    def step_line(j):
        n, w = pieces[j]
        landed(zr.at[pl.ds(1, DH - 1), pl.ds(n, w)], z_sem.at[j])
        for u in range(n, n + w):
            value = fv[u, dh]
            for k, pd in line:
                value = value + zr[k, u].astype(f32)
            if u < n2:
                g2_ref[:, u * U : (u + 1) * U] = value
            else:
                g1_ref[:, (u - n2) * U : (u - n2 + 1) * U] = value

    def back(rows, at, units):
        cols = pl.ds(at * U, units * U)
        value = lax.dot_general(
            og_v[rows, :], w2_v[cols, :], (((1,), (1,)), ((), ())), preferred_element_type=f32
        )
        keep = h_v[rows, cols].astype(f32) > 0
        dh_v[rows, cols] = jnp.where(keep, value, jnp.zeros_like(value)).astype(bf16)

    E = tab_ref.shape[1]
    tile = 256
    every = pl.ds(0, tokens)

    def table_tiles(a, first, last):
        def body(t, _):
            start = pl.multiple_of(t * tile, tile)
            rows = pl.ds(start, tile)
            wanted = start + lax.broadcasted_iota(jnp.int32, (tile, LANES), 0)
            total = sums[rows, :] if a else jnp.zeros((tile, E), f32)
            for k in range(1, DH) if a else range(1):
                parts, blocks = [], []
                for ids, block in ((iz[k], eb[k]) if k else (iw[dh], sb[dh]), (io[k], eo[k])):
                    for e in range(GX):
                        hit = wanted == jnp.maximum(ids[e, 0], ids[e, 1])
                        parts.append(jnp.where(hit, 1.0, 0.0).astype(bf16))
                    blocks.append(block.reshape(GX * LANES, E))
                total = total + jnp.dot(
                    jnp.concatenate(parts, axis=1),
                    jnp.concatenate(blocks, axis=0),
                    preferred_element_type=f32,
                )
            if not a:
                sums[rows, :] = total
            else:
                state = st_ref[rows, :] + total * total
                st_ref[rows, :] = state
                tab_ref[rows, :] = tab_ref[rows, :] - learn_rate * total / (jnp.sqrt(state) + epsilon)
            return 0

        lax.fori_loop(first, last, body, 0)

    tiles = tab_ref.shape[0] // tile
    some = tiles // 4
    n2 = og_v.shape[1] // U
    n1 = dh_v.shape[1] // U
    assert n2 == 4 and n1 == 8
    loads[("og", 0)].wait()
    for k in range(GX):
        loads[("h", "away", 0, k)].wait()
    product(cs, other_c, 0, 4, h_v, True, og_v, 0, pl.ds(0, half))
    loads[("og", 1)].wait()
    for k in range(GX):
        loads[("h", "away", 1, k)].wait()
    product(cs, other_c, 0, 4, h_v, True, og_v, 0, pl.ds(half, half), True)
    send_core(0, 0, 2)
    send_core(1, 2, 2)
    for k in range(GX):
        loads[("h", "home", k)].wait()
    product(hv, c, 0, 4, h_v, True, og_v, 0)
    chip_landed(0, 0, 2)
    step_chip(0)
    loads["w2"].wait()
    back(every, 0, 4)
    chip_landed(1, 2, 2)
    line_first(8)
    step_chip(1)
    loads["x"].wait()
    away_two(2, 4, x_v, dh_v, 0)
    slots_line()
    product(hv, c, 4, 4, x_v, False, dh_v, 0)
    chip_landed(2, 4, 2)
    step_chip(2)
    step_first(0)
    back(every, 4, 4)
    chip_landed(3, 6, 2)
    step_chip(3)
    step_first(1)
    away_two(4, 8, x_v, dh_v, 4)
    product(hv, c, 8, 4, x_v, False, dh_v, 4)
    chip_landed(4, 8, 2)
    step_chip(4)
    step_chip(5)
    chip_landed(5, 10, 2)
    step_plane(6)
    line_first(7)
    step_first(2)
    step_second(0)
    step_second(1)
    slots_here(0)
    table_tiles(0, 0, 2 * some)
    step_first(3)
    line_plane(8)
    table_tiles(0, 2 * some, 4 * some)
    slots_core()
    step_first(4)
    step_first(5)
    step_second(2)
    loads["tab"].wait()
    loads["st"].wait()
    step_second(3)
    plane_landed(6)
    step_second(4)
    line_plane(7)
    step_second(5)
    slots_here(1)
    table_tiles(1, 0, tiles)
    for j in range(7):
        step_line(j)
    line_end(8)
    line_end(7)
    for i in range(3):
        left_here(ij.at[0], 2 * i)
        left_here(sb.at[:, 0, 0], 2 * i + 1)
    left_here(iz.at[rest], 12)
    left_here(eb.at[rest], 13)
    left_here(iz.at[0], 14)
    left_here(eb.at[0], 15)
    left_here(iz.at[rest], 16)
    left_here(eb.at[rest], 17)
    left_here(cs, 8)
    left_here(xs.at[pl.ds(0, units[0])], 9)
    left_here(ys.at[pl.ds(0, units[0])], 10)
    left_here(ds, 18)
    left_here(zx.at[:, pl.ds(1, DH - 1)], 19)
    left_here(px, 20)
    left_here(zs.at[pl.ds(1, DH - 1), pl.ds(0, units[1])], 11)


def store(*refs):
    ins, outs, sems = refs[:4], refs[4:8], refs[8]
    copies = []
    for a, b in zip(ins, outs):
        parts = sems.shape[0] // 4
        rows = a.shape[0] // parts
        for i in range(parts):
            at = pl.ds(i * rows, rows)
            copies.append(pltpu.make_async_copy(a.at[at], b.at[at], sems.at[len(copies)]))
    for copy in copies[::-1]:
        copy.start()
    for copy in copies:
        copy.wait()


def solution(mesh):
    G, D = mesh.shape["grp"], mesh.shape["dev"]

    def on_device(
        layer_input, hidden_pre, out_grad, second_weight,
        row_grads, row_ids, block_counts, emb_table, adagrad_state,
    ):
        T, IN = layer_input.shape
        HID, OUT = second_weight.shape
        E = row_grads.shape[1]
        cap = row_grads.shape[0] // D
        assert LANES // cap == 2
        GX, DH = G // 2, D // 2
        R1, R2 = IN // (G * D), HID // (G * D)
        assert R1 == R2
        U = LANES
        N = (OUT + HID) // U
        hbm = pl.BlockSpec(memory_space=pltpu.HBM)
        vmem = pl.BlockSpec(memory_space=pltpu.VMEM)
        dma = pltpu.SemaphoreType.DMA
        operands = (
            layer_input, hidden_pre, out_grad, second_weight,
            row_grads.reshape(DH, 2, cap, E), row_ids.reshape(DH, LANES), block_counts,
            emb_table, adagrad_state,
        )
        grads = pl.pallas_call(
            functools.partial(kernel, G, D),
            out_shape=[
                jax.ShapeDtypeStruct((R1, HID), f32),
                jax.ShapeDtypeStruct((R2, OUT), f32),
                jax.ShapeDtypeStruct(emb_table.shape, f32),
                jax.ShapeDtypeStruct(adagrad_state.shape, f32),
            ],
            in_specs=[hbm] * 9,
            out_specs=[vmem] * 4,
            scratch_shapes=[
                pltpu.VMEM((T, IN), bf16),
                pltpu.VMEM((T, HID), bf16),
                pltpu.VMEM((T, OUT), bf16),
                pltpu.VMEM((HID, OUT), bf16),
                pltpu.VMEM((T, HID), bf16),
                pltpu.VMEM((DH, LANES), jnp.int32),
                pltpu.SMEM((D,), jnp.int32),
                pltpu.VMEM((N, GX, D * R1, U), f32),
                pltpu.VMEM((N, GX, D * R1, U), f32),
                pltpu.VMEM((N, GX, D * R1, U), f32),
                pltpu.VMEM((N, 2, DH, R1, U), bf16),
                pltpu.VMEM((N, 2, DH, R1, U), bf16),
                pltpu.VMEM((N, DH, R1, U), bf16),
                pltpu.VMEM((N, DH, R1, U), bf16),
                pltpu.VMEM((N, DH, R1, U), f32),
                pltpu.VMEM((DH, N, R1, U), bf16),
                pltpu.VMEM((DH, N, R1, U), bf16),
                pltpu.VMEM((3, 1, 1, DH, R1, U), bf16),
                pltpu.VMEM((3, 1, 1, DH, R1, U), bf16),
                pltpu.VMEM((2, DH, 2, 2, R1, U), bf16),
                pltpu.VMEM((2, DH, 2, 2, R1, U), bf16),
                pltpu.VMEM((2, R1, U), f32),
                pltpu.VMEM((2, 3, R1, U), bf16),
                pltpu.VMEM((2, 3, R1, U), bf16),
                pltpu.VMEM((DH, GX, 2, cap, E), bf16),
                pltpu.VMEM((DH, GX, 2, cap, E), bf16),
                pltpu.VMEM((DH, GX, 2, cap, E), bf16),
                pltpu.VMEM((2, DH, 1, LANES), jnp.int32),
                pltpu.VMEM((DH, GX, 2, 1, LANES), jnp.int32),
                pltpu.VMEM((DH, GX, 2, 1, LANES), jnp.int32),
                pltpu.VMEM((DH, GX, 2, 1, LANES), jnp.int32),
                pltpu.VMEM(emb_table.shape, f32),
                dma((15,)),
                dma((21,)),
                dma((6,)), dma((9,)), dma((9,)), dma((9,)),
                dma((12,)),
                dma((3, 1 + 2)),
            ],
            compiler_params=pltpu.CompilerParams(
                collective_id=0, has_side_effects=True, vmem_limit_bytes=48 * 1024 * 1024
            ),
        )(*[pltpu.with_memory_space_constraint(a, pltpu.HBM) for a in operands])
        return pl.pallas_call(
            store,
            out_shape=[jax.ShapeDtypeStruct(a.shape, a.dtype) for a in grads],
            in_specs=[vmem] * 4,
            out_specs=[hbm] * 4,
            scratch_shapes=[dma((4 * 1,))],
            compiler_params=pltpu.CompilerParams(vmem_limit_bytes=8 * 1024 * 1024),
        )(*grads)

    return jax.shard_map(
        on_device,
        mesh=mesh,
        in_specs=(
            P(("grp", "dev"), None),
            P(("grp", "dev"), None),
            P(("grp", "dev"), None),
            P(),
            P(("grp", "dev"), None),
            P(("grp", "dev")),
            P(("grp", "dev")),
            P("dev", None),
            P("dev", None),
        ),
        out_specs=(P(("grp", "dev"), None), P(("grp", "dev"), None), P("dev", None), P("dev", None)),
        check_vma=False,
    )
```
